32 devices in a mesh: blk: 16 (over z, y, x), grp: 2 (over core).
Axes of the slice: x: 2, y: 2, z: 4, core: 2. Of those that a mesh axis runs over, the one named last changes fastest.
Arguments:
- sky_maps: float32 [4, 128, 4096], P(None, ('blk', 'grp')), may hold values from -6 to 6
- legendre: bfloat16 [128, 512, 2048], P(('blk', 'grp')), may hold values from -0.5 to 0.5
- owner_table: int32 [512], replicated, may hold values from 0 to 511, each once
Outputs:
- harmonics: float32 [512, 4, 2, 2048], P(('blk', 'grp'))
- spectra: float32 [10, 2048], P(None, ('blk', 'grp'))
The draws below stay inside these ranges and needn't reach their ends.
Inputs may be any that keep to these rules, and one draw needn't show every extreme that they name: `owner_table`: a permutation of the orders 0 to 511.
All inputs are finite; a program needn't handle non-finite values.
Results may differ from the reference program's by a relative error of at most 0.0034.
Values may be sent and summed in bfloat16 or wider, within the bound.
A program may use at most 128 MiB of HBM per device.

```python
import math
import jax
import jax.numpy as jnp
import numpy as np
from jax import lax

MAPS = 4
M = 512
L = 2048
NPHI = 4096
CYCLES = 128


def levels(own_key, shape, shards, smallest, top_value):
    def one(dim, blocks):
        heights = jax.random.uniform(jax.random.fold_in(jax.random.fold_in(own_key, 6), dim), (blocks,), jnp.float32, smallest / len(shards), top_value / len(shards))
        return jnp.repeat(jnp.exp(heights), shape[dim] // blocks).reshape((-1,) + (1,) * (len(shape) - dim - 1))

    loudness = one(*shards[0])
    for cut in shards[1:]:
        loudness = loudness * one(*cut)
    return loudness


def scatter_about(own_key, dims, scale, limit, pieces=(), kind=jnp.bfloat16):
    array = scale * jax.random.normal(own_key, dims, jnp.float32)
    if pieces:
        array = array * levels(own_key, dims, pieces, -0.22, 0.18)
    return jnp.clip(array, -limit, limit).astype(kind)


def setup_inputs(seed: int = 0) -> dict:
    seeds = jax.random.split(jax.random.key(seed), 4)
    sky_maps = scatter_about(seeds[0], (MAPS, CYCLES, NPHI), 1.0, 6.0, ((1, 32),), jnp.float32)
    legendre = scatter_about(seeds[1], (CYCLES, M, L), CYCLES ** -0.5, 0.5, ((0, 32),))
    owner_table = jax.random.permutation(seeds[2], M).astype(jnp.int32)
    return dict(sky_maps=sky_maps, legendre=legendre, owner_table=owner_table)


def reference(sky_maps, legendre, owner_table):
    coeffs = jnp.fft.rfft(sky_maps, axis=-1)[..., :M] / math.sqrt(NPHI)
    fourier = jnp.stack([jnp.real(coeffs), jnp.imag(coeffs)], axis=2)
    fourier = jnp.transpose(fourier, (1, 0, 2, 3)).reshape(CYCLES, 2 * MAPS, M).astype(jnp.bfloat16)
    ell_index = jnp.arange(L, dtype=jnp.int32)

    def per_block(orders):
        table = jnp.take(legendre, orders, axis=1).astype(jnp.float32)
        values = jnp.take(fourier, orders, axis=2).astype(jnp.float32)
        block = jnp.einsum('rcm,rml->mcl', values, table)
        keep = ell_index[None, None, :] >= orders[:, None, None]
        return jnp.where(keep, block, jnp.zeros_like(block))
    harmonics = lax.map(per_block, owner_table.reshape(M // 64, 64)).reshape(M, MAPS, 2, L)
    weight = jnp.where(owner_table == 0, jnp.float32(1.0), jnp.float32(2.0)).astype(jnp.float32)
    cross = jnp.einsum('m,miql,mjql->ijl', weight, harmonics, harmonics)
    first, second = np.triu_indices(MAPS)
    spectra = cross[first, second] / (2 * ell_index + 1).astype(jnp.float32)
    return (harmonics, spectra)
```

```python
import functools
import math

import jax
import jax.numpy as jnp
import numpy as np
from jax import lax
from jax.experimental import pallas as pl
from jax.experimental.pallas import tpu as pltpu
from jax.sharding import PartitionSpec as P

AXES = ("blk", "grp")
CHUNKS = 4
PLANE = 8
VMEM_LIMIT = 56 * 1024 * 1024


def kernel_call(body, out_shape, *, grid, in_specs, out_specs, flops, traffic):
    return pl.pallas_call(
        body,
        out_shape=out_shape,
        grid=grid,
        in_specs=in_specs,
        out_specs=out_specs,
        compiler_params=pltpu.CompilerParams(vmem_limit_bytes=VMEM_LIMIT),
        cost_estimate=pl.CostEstimate(flops=flops, bytes_accessed=traffic, transcendentals=0),
    )


def split_bf16(values):
    high = values.astype(jnp.bfloat16)
    low = (values - high.astype(jnp.float32)).astype(jnp.bfloat16)
    return high, low


def dot3(left, right_high, right_low):
    high, low = split_bf16(left)
    dot = functools.partial(jnp.dot, preferred_element_type=jnp.float32)
    return dot(high, right_high) + (dot(high, right_low) + dot(low, right_high))


def fourier_tables(pixels, order_count, width):
    coarse = pixels // width
    k1, m1 = np.meshgrid(np.arange(coarse), np.arange(coarse), indexing="ij")
    angle = 2.0 * math.pi * ((k1 * m1) % coarse) / coarse
    first = np.concatenate([np.cos(angle.T), -np.sin(angle.T)], axis=0)
    k2 = np.arange(width)[:, None]
    m = np.arange(order_count)[None, :]
    angle = 2.0 * math.pi * ((k2 * m) % pixels) / pixels
    cosine, sine = np.cos(angle) / math.sqrt(pixels), np.sin(angle) / math.sqrt(pixels)
    second = np.block([[cosine, -sine], [sine, cosine]]).astype(np.float32)
    high = second.astype(jnp.bfloat16)
    low = (second - high.astype(np.float32)).astype(jnp.bfloat16)
    return first.astype(np.float32), high, low


def fourier_body(rows, coarse, width, x_ref, first_ref, high_ref, low_ref, hot_ref, out_ref):
    order_count = hot_ref.shape[1]
    columns = 2 * order_count
    m1 = lax.broadcasted_iota(jnp.int32, (coarse, columns), 0)
    col = lax.broadcasted_iota(jnp.int32, (coarse, columns), 1)
    keep = (col % coarse) == m1
    first = first_ref[...]
    picked = []
    for b in range(rows):
        stage = jnp.dot(
            first,
            x_ref[b * coarse : (b + 1) * coarse, :],
            precision=lax.Precision.HIGHEST,
            preferred_element_type=jnp.float32,
        )
        both = jnp.concatenate([stage[:coarse], stage[coarse:]], axis=1)
        full = dot3(both, high_ref[...], low_ref[...])
        picked.append(jnp.sum(jnp.where(keep, full, 0.0), axis=0, keepdims=True))
    spectral = jnp.concatenate(picked, axis=0).astype(jnp.bfloat16)
    for part in range(2):
        out_ref[part] = lax.dot_general(
            spectral[:, part * order_count : (part + 1) * order_count],
            hot_ref[...],
            (((1,), (1,)), ((), ())),
            preferred_element_type=jnp.float32,
        ).astype(jnp.bfloat16)


def owned_fourier(sky_maps, one_hot):
    maps, cycles, pixels = sky_maps.shape
    slots, order_count = one_hot.shape
    width = 128
    coarse = pixels // width
    rows = maps * cycles
    first, high, low = fourier_tables(pixels, order_count, width)
    vmem = pl.BlockSpec(memory_space=pltpu.VMEM)
    return pl.pallas_call(
        functools.partial(fourier_body, rows, coarse, width),
        out_shape=jax.ShapeDtypeStruct((2, rows, slots), jnp.bfloat16),
        in_specs=[vmem] * 5,
        out_specs=vmem,
        compiler_params=pltpu.CompilerParams(vmem_limit_bytes=VMEM_LIMIT),
        cost_estimate=pl.CostEstimate(
            flops=6 * rows * coarse * 2 * width * 2 * order_count,
            bytes_accessed=4 * sky_maps.size + 8 * width * order_count,
            transcendentals=0,
        ),
    )(
        sky_maps.reshape(rows * coarse, width),
        jnp.asarray(first),
        jnp.asarray(high),
        jnp.asarray(low),
        one_hot,
    )


def permute_body(per_chunk, hot_ref, table_ref, *out_refs):
    picked = jnp.dot(hot_ref[...], table_ref[0], preferred_element_type=jnp.float32)
    picked = picked.astype(jnp.bfloat16)
    for c, out_ref in enumerate(out_refs):
        out_ref[0] = picked[c * per_chunk : (c + 1) * per_chunk]


def permute_rows(one_hot, half, legendre):
    cycles, orders, ells = legendre.shape
    rows = one_hot.shape[0] // 2
    per_chunk = rows // CHUNKS
    tile = ells // 2
    return kernel_call(
        functools.partial(permute_body, per_chunk),
        [jax.ShapeDtypeStruct((cycles, per_chunk, ells), jnp.bfloat16)] * CHUNKS,
        grid=(cycles, ells // tile),
        in_specs=[
            pl.BlockSpec((rows, orders), lambda r, t: (half, 0)),
            pl.BlockSpec((1, orders, tile), lambda r, t: (r, 0, t)),
        ],
        out_specs=[pl.BlockSpec((1, per_chunk, tile), lambda r, t: (r, 0, t))] * CHUNKS,
        flops=2 * rows * orders * ells * cycles,
        traffic=2 * legendre.size + 2 * cycles * rows * ells,
    )(one_hot, legendre)


def group_partial(size, coef_ref, own_ref, got_ref):
    cycles = own_ref.shape[0]
    depth = 2 * cycles * size
    tile = own_ref.shape[2]
    values = jnp.concatenate(
        [own_ref[...].reshape(cycles * size, tile), got_ref[...].reshape(cycles * size, tile)], axis=0
    )
    coef = coef_ref[0].astype(jnp.float32)
    channels = coef.shape[0]
    spread = jnp.broadcast_to(coef[None], (size, channels, depth)).reshape(size * channels, depth)
    row = lax.broadcasted_iota(jnp.int32, (size * channels, depth), 0) // channels
    col = lax.broadcasted_iota(jnp.int32, (size * channels, depth), 1) % size
    left = jnp.where(row == col, spread, 0.0).astype(jnp.bfloat16)
    return jnp.dot(left, values, preferred_element_type=jnp.float32)


def send_body(size, coef_ref, own_ref, got_ref, *rest):
    *add_refs, out_ref = rest
    total = group_partial(size, coef_ref, own_ref, got_ref)
    for add_ref in add_refs:
        total = total + add_ref[...].astype(jnp.float32)
    out_ref[...] = total.astype(out_ref.dtype)


def last_body(size, coef_ref, own_ref, got_ref, x_ref, y_ref, keep_ref, *send_refs):
    total = group_partial(size, coef_ref, own_ref, got_ref)
    total = total + x_ref[...].astype(jnp.float32) + y_ref[...].astype(jnp.float32)
    rows = keep_ref.shape[0]
    keep_ref[...] = total[:rows]
    for k, send_ref in enumerate(send_refs):
        send_ref[...] = total[(k + 1) * rows : (k + 2) * rows].astype(send_ref.dtype)


def stage_specs(size, channels, cycles, tile, coef_base, base):
    return [
        pl.BlockSpec((1, channels, 2 * cycles * size), lambda g, t: (coef_base + base + g, 0, 0)),
        pl.BlockSpec((cycles, size, tile), lambda g, t: (0, base + g, t)),
        pl.BlockSpec((cycles, size, tile), lambda g, t: (0, base + g, t)),
    ]


def send_stage(size, coef, coef_base, base, groups, own, got, adds):
    cycles, _, ells = own.shape
    channels = coef.shape[1]
    tile = ells // 2
    rows = size * channels
    return kernel_call(
        functools.partial(send_body, size),
        jax.ShapeDtypeStruct((groups * rows, ells), jnp.bfloat16),
        grid=(groups, ells // tile),
        in_specs=stage_specs(size, channels, cycles, tile, coef_base, base)
        + [pl.BlockSpec((rows, tile), functools.partial(lambda f, g, t: (f + g, t), first)) for _, first in adds],
        out_specs=pl.BlockSpec((rows, tile), lambda g, t: (g, t)),
        flops=2 * groups * rows * 2 * cycles * size * ells,
        traffic=groups * (4 * cycles * size + 2 * rows * (1 + len(adds))) * ells,
    )(coef, own, got, *[add for add, _ in adds])


def last_stage(size, columns, coef, coef_base, own, got, from_first, from_second):
    cycles, _, ells = own.shape
    channels = coef.shape[1]
    tile = ells // 2
    rows = size * channels
    part = rows // columns
    block = pl.BlockSpec((rows, tile), lambda g, t: (0, t))
    out_block = pl.BlockSpec((part, tile), lambda g, t: (0, t))
    return kernel_call(
        functools.partial(last_body, size),
        [jax.ShapeDtypeStruct((part, ells), jnp.float32)]
        + [jax.ShapeDtypeStruct((part, ells), jnp.bfloat16)] * (columns - 1),
        grid=(1, ells // tile),
        in_specs=stage_specs(size, channels, cycles, tile, coef_base, 0) + [block, block],
        out_specs=[out_block] * columns,
        flops=2 * rows * 2 * cycles * size * ells,
        traffic=(4 * cycles * size + 8 * rows) * ells,
    )(coef, own, got, from_first, from_second)


def finish_body(columns, maps, tile, order_ref, *refs):
    ins, (harm_ref, power_ref) = refs[:-2], refs[-2:]
    channels = 2 * maps
    start = pl.program_id(0) * tile
    total = [None] * maps
    part = ins[0].shape[0]
    ell = start + lax.broadcasted_iota(jnp.int32, (part, tile), 1)
    for c in range(CHUNKS):
        mine = ins[c * columns : (c + 1) * columns]
        value = mine[0][...]
        for other in mine[1:]:
            value = value + other[...].astype(jnp.float32)
        order = order_ref[c * part : (c + 1) * part, 0:1]
        value = jnp.where(ell >= order, value, 0.0)
        harm_ref[c * part : (c + 1) * part, :] = value
        weighted = jnp.where(order == 0, value, 2.0 * value)
        for s in range(part // channels):
            mode = value[s * channels : (s + 1) * channels]
            heavy = weighted[s * channels : (s + 1) * channels]
            for k in range(maps // 2 + 1):
                turned = mode if k == 0 else jnp.concatenate([mode[2 * k :], mode[: 2 * k]], axis=0)
                term = heavy * turned
                total[k] = term if total[k] is None else total[k] + term
    pair = 0
    for i in range(maps):
        for j in range(i, maps):
            k, a = (j - i, i) if j - i <= maps // 2 else (maps - (j - i), j)
            power_ref[pair : pair + 1, :] = total[k][2 * a : 2 * a + 1] + total[k][2 * a + 1 : 2 * a + 2]
            pair += 1


def finish(columns, maps, orders, parts):
    ells = parts[0].shape[1]
    part = parts[0].shape[0]
    tile = ells // 4
    pairs = maps * (maps + 1) // 2
    rows = part * CHUNKS
    return kernel_call(
        functools.partial(finish_body, columns, maps, tile),
        [jax.ShapeDtypeStruct((rows, ells), jnp.float32), jax.ShapeDtypeStruct((pairs, ells), jnp.float32)],
        grid=(ells // tile,),
        in_specs=[pl.BlockSpec((rows, 128), lambda t: (0, 0))]
        + [pl.BlockSpec((part, tile), lambda t: (0, t))] * len(parts),
        out_specs=[pl.BlockSpec((rows, tile), lambda t: (0, t)), pl.BlockSpec((pairs, tile), lambda t: (0, t))],
        flops=20 * rows * ells,
        traffic=4 * rows * ells * 4,
    )(orders, *parts)


def per_device(sky_maps, legendre, owner_table):
    maps = sky_maps.shape[0]
    cycles, order_count, ells = legendre.shape
    devices = lax.axis_size(AXES)
    columns = devices // PLANE
    own_count = order_count // devices
    share = own_count // CHUNKS
    size = columns * share
    channels = 2 * maps
    me = lax.axis_index(AXES)

    core, chunk, one, two, step, item = np.indices((2, CHUNKS, 2, 2, columns, share)).reshape(6, -1)
    swap = chunk % 2 == 1
    low = core + 2 * np.where(swap, two, one) + 4 * np.where(swap, one, two)
    member = (me % PLANE) ^ jnp.asarray(low, jnp.int32)
    column = (me // PLANE + jnp.asarray(step, jnp.int32)) % columns
    slot = (column * PLANE + member) * own_count + jnp.asarray(chunk * share + item, jnp.int32)
    index = lax.iota(jnp.int32, order_count)
    order = jnp.sum(jnp.where(slot[:, None] == index[None, :], owner_table[None, :], 0), axis=1)
    one_hot = (order[:, None] == index[None, :]).astype(jnp.bfloat16)

    def swap_with(value, bit):
        return lax.ppermute(value, AXES, [(d, d ^ bit) for d in range(devices)])

    outgoing = permute_rows(one_hot, 1, legendre)
    got = [swap_with(value, 1) for value in outgoing]
    four = owned_fourier(sky_maps, one_hot)
    half = order_count // 2
    own = permute_rows(one_hot, 0, legendre)
    coef = jnp.stack([four[:, :, :half], swap_with(four[:, :, half:], 1)])
    coef = coef.reshape(2, 2, maps, cycles, half // size, size)
    coef = jnp.transpose(coef, (4, 2, 1, 0, 3, 5)).reshape(half // size, channels, 2 * cycles * size)

    bits = [(2, 4) if c % 2 == 0 else (4, 2) for c in range(CHUNKS)]
    first = [
        swap_with(send_stage(size, coef, 4 * c, 2, 2, own[c], got[c], []), bits[c][0]) for c in range(CHUNKS)
    ]
    second = [
        swap_with(send_stage(size, coef, 4 * c, 1, 1, own[c], got[c], [(first[c], 1)]), bits[c][1])
        for c in range(CHUNKS)
    ]
    parts = []
    for c in range(CHUNKS):
        keep, *sends = last_stage(size, columns, coef, 4 * c, own[c], got[c], first[c], second[c])
        parts.append(keep)
        for k, send in enumerate(sends):
            ring = [(d, (d + (k + 1) * PLANE) % devices) for d in range(devices)]
            parts.append(lax.ppermute(send, AXES, ring))

    owned = lax.dynamic_slice_in_dim(owner_table, me * own_count, own_count)
    orders = jnp.broadcast_to(owned[:, None, None], (own_count, channels, 128)).reshape(-1, 128)
    harmonics, power = finish(columns, maps, orders, parts)
    harmonics = harmonics.reshape(own_count, maps, 2, ells)
    ell_share = ells // devices
    spread = power.reshape(power.shape[0], devices, ell_share).transpose(1, 0, 2)
    shares = lax.all_to_all(spread, AXES, split_axis=0, concat_axis=0, tiled=True)
    owned_ells = me * ell_share + lax.iota(jnp.int32, ell_share)
    spectra = jnp.sum(shares, axis=0) / (2 * owned_ells + 1).astype(jnp.float32)[None, :]
    return (harmonics, spectra)


def solution(mesh):
    return jax.shard_map(
        per_device,
        mesh=mesh,
        in_specs=(P(None, AXES, None), P(AXES, None, None), P()),
        out_specs=(P(AXES, None, None, None), P(None, AXES)),
        check_vma=False,
    )
```

```python
import functools
import math

import jax
import jax.numpy as jnp
import numpy as np
from jax import lax
from jax.experimental import pallas as pl
from jax.experimental.pallas import tpu as pltpu
from jax.sharding import PartitionSpec as P

AXES = ("blk", "grp")
CHUNKS = 8
PLANE = 8
MIB = 1024 * 1024


def kernel_call(body, out_shape, *, grid, in_specs, out_specs, flops, traffic, vmem=28):
    return pl.pallas_call(
        body,
        out_shape=out_shape,
        grid=grid,
        in_specs=in_specs,
        out_specs=out_specs,
        compiler_params=pltpu.CompilerParams(vmem_limit_bytes=vmem * MIB),
        cost_estimate=pl.CostEstimate(flops=flops // 1000, bytes_accessed=traffic // 1000, transcendentals=0),
    )


def split_bf16(values):
    high = values.astype(jnp.bfloat16)
    low = (values - high.astype(jnp.float32)).astype(jnp.bfloat16)
    return high, low


def dot3(left, right_high, right_low):
    high, low = split_bf16(left)
    dot = functools.partial(jnp.dot, preferred_element_type=jnp.float32)
    return dot(high, right_high) + (dot(high, right_low) + dot(low, right_high))


def ordered(body, after, in_specs, operands):
    if after is None:
        return body, in_specs, operands
    return (lambda _, *refs: body(*refs)), [pl.BlockSpec(memory_space=pl.ANY)] + in_specs, [after] + operands


def fourier_tables(pixels, order_count, width):
    coarse = pixels // width
    k1, m1 = np.meshgrid(np.arange(coarse), np.arange(coarse), indexing="ij")
    angle = 2.0 * math.pi * ((k1 * m1) % coarse) / coarse
    first = np.concatenate([np.cos(angle.T), -np.sin(angle.T)], axis=0)
    k2 = np.arange(width)[:, None]
    m = np.arange(order_count)[None, :]
    angle = 2.0 * math.pi * ((k2 * m) % pixels) / pixels
    cosine, sine = np.cos(angle) / math.sqrt(pixels), np.sin(angle) / math.sqrt(pixels)
    second = np.block([[cosine, -sine], [sine, cosine]]).astype(np.float32)
    high = second.astype(jnp.bfloat16)
    low = (second - high.astype(np.float32)).astype(jnp.bfloat16)
    return first.astype(np.float32), high, low


def fourier_body(rows, coarse, x_ref, first_ref, high_ref, low_ref, hot_ref, out_ref):
    order_count = hot_ref.shape[1]
    columns = 2 * order_count
    m1 = lax.broadcasted_iota(jnp.int32, (1, coarse, columns), 1)
    col = lax.broadcasted_iota(jnp.int32, (1, coarse, columns), 2)
    keep = (col % coarse) == m1
    first = first_ref[...]
    stages = []
    for b in range(rows):
        stage = jnp.dot(
            first,
            x_ref[b * coarse : (b + 1) * coarse, :],
            precision=lax.Precision.HIGHEST,
            preferred_element_type=jnp.float32,
        )
        stages.append(jnp.concatenate([stage[:coarse], stage[coarse:]], axis=1))
    full = dot3(jnp.concatenate(stages, axis=0), high_ref[...], low_ref[...])
    full = full.reshape(rows, coarse, columns)
    spectral = jnp.sum(jnp.where(keep, full, 0.0), axis=1).astype(jnp.bfloat16)
    for part in range(2):
        out_ref[part] = lax.dot_general(
            spectral[:, part * order_count : (part + 1) * order_count],
            hot_ref[...],
            (((1,), (1,)), ((), ())),
            preferred_element_type=jnp.float32,
        ).astype(jnp.bfloat16)


def owned_fourier(sky_maps, one_hot):
    maps, cycles, pixels = sky_maps.shape
    slots, order_count = one_hot.shape
    width = 128
    coarse = pixels // width
    rows = maps * cycles
    first, high, low = fourier_tables(pixels, order_count, width)
    vmem = pl.BlockSpec(memory_space=pltpu.VMEM)
    return pl.pallas_call(
        functools.partial(fourier_body, rows, coarse),
        out_shape=jax.ShapeDtypeStruct((2, rows, slots), jnp.bfloat16),
        in_specs=[vmem] * 5,
        out_specs=vmem,
        compiler_params=pltpu.CompilerParams(vmem_limit_bytes=32 * MIB),
        cost_estimate=pl.CostEstimate(
            flops=6 * rows * coarse * 2 * width * 2 * order_count,
            bytes_accessed=4 * sky_maps.size + 8 * width * order_count,
            transcendentals=0,
        ),
    )(
        sky_maps.reshape(rows * coarse, width),
        jnp.asarray(first),
        jnp.asarray(high),
        jnp.asarray(low),
        one_hot,
    )


def permute_body(per_pair, hot_ref, table_ref, *out_refs):
    picked = jnp.dot(hot_ref[...], table_ref[0], preferred_element_type=jnp.float32)
    picked = picked.astype(jnp.bfloat16)
    for c, out_ref in enumerate(out_refs):
        out_ref[0] = picked[c * per_pair : (c + 1) * per_pair]


def permute_rows(one_hot, block, pairs, per_pair, legendre, after=None):
    cycles, orders, ells = legendre.shape
    rows = pairs * per_pair
    tile = ells // 2
    in_specs = [
        pl.BlockSpec((rows, orders), lambda r, t: (block, 0)),
        pl.BlockSpec((1, orders, tile), lambda r, t: (r, 0, t)),
    ]
    body = functools.partial(permute_body, per_pair)
    body, in_specs, operands = ordered(body, after, in_specs, [one_hot, legendre])
    return kernel_call(
        body,
        [jax.ShapeDtypeStruct((cycles, per_pair, ells), jnp.bfloat16)] * pairs,
        grid=(cycles, ells // tile),
        in_specs=in_specs,
        out_specs=[pl.BlockSpec((1, per_pair, tile), lambda r, t: (r, 0, t))] * pairs,
        flops=2 * rows * orders * ells * cycles,
        traffic=2 * legendre.size + 2 * cycles * rows * ells,
    )(*operands)


def block_partial(wide, block, first, count, coef_ref, own_ref, got_ref):
    cycles, _, tile = own_ref.shape
    depth = 2 * cycles * wide
    picked = slice(block * wide, (block + 1) * wide)
    values = jnp.concatenate(
        [ref[:, picked, :].reshape(cycles * wide, tile) for ref in (own_ref, got_ref)], axis=0
    )
    coef = coef_ref[block].astype(jnp.float32)
    channels = coef.shape[0]
    rows = count * channels
    spread = jnp.broadcast_to(coef[None], (count, channels, depth)).reshape(rows, depth)
    row = lax.broadcasted_iota(jnp.int32, (rows, depth), 0) // channels + first
    col = lax.broadcasted_iota(jnp.int32, (rows, depth), 1) % wide
    left = jnp.where(row == col, spread, 0.0).astype(jnp.bfloat16)
    return jnp.dot(left, values, preferred_element_type=jnp.float32)


def first_body(wide, coef_ref, own_ref, got_ref, *out_refs):
    for side, out_ref in enumerate(out_refs):
        total = block_partial(wide, 2 * side + 1, 0, wide, coef_ref, own_ref, got_ref)
        out_ref[...] = total.astype(out_ref.dtype)


def second_body(wide, coef_ref, own_ref, got_ref, *refs):
    size = wide // 2
    for side, (add_ref, out_ref) in enumerate(zip(refs[:2], refs[2:])):
        total = block_partial(wide, 2 * side, size, size, coef_ref, own_ref, got_ref)
        out_ref[...] = (total + add_ref[...].astype(jnp.float32)).astype(out_ref.dtype)


def last_body(wide, coef_ref, own_ref, got_ref, *refs):
    size = wide // 2
    adds, keep_ref, send_refs = refs[:4], refs[4], refs[5:]
    part = keep_ref.shape[0] // 2
    for side in range(2):
        total = block_partial(wide, 2 * side, 0, size, coef_ref, own_ref, got_ref)
        total = total + adds[side][...].astype(jnp.float32) + adds[2 + side][...].astype(jnp.float32)
        keep_ref[side * part : (side + 1) * part, :] = total[:part]
        for k, send_ref in enumerate(send_refs):
            piece = total[(k + 1) * part : (k + 2) * part]
            send_ref[side * part : (side + 1) * part, :] = piece.astype(send_ref.dtype)


def pair_stage(body, wide, pair, coef, own, got, adds, outs, after):
    cycles, slots, ells = own.shape
    channels = coef.shape[1]
    tile = ells // 2
    table = pl.BlockSpec((cycles, slots, tile), lambda t: (0, 0, t))
    in_specs = [pl.BlockSpec((4, channels, 2 * cycles * wide), lambda t: (pair, 0, 0)), table, table]
    for _, at, rows in adds:
        in_specs.append(pl.BlockSpec((rows, tile), functools.partial(lambda at, t: (at, t), at)))
    operands = [coef, own, got] + [add for add, _, _ in adds]
    body, in_specs, operands = ordered(functools.partial(body, wide), after, in_specs, operands)
    return kernel_call(
        body,
        [jax.ShapeDtypeStruct((rows, ells), dtype) for rows, dtype in outs],
        grid=(ells // tile,),
        in_specs=in_specs,
        out_specs=[pl.BlockSpec((rows, tile), lambda t: (0, t)) for rows, _ in outs],
        flops=2 * 4 * cycles * wide * wide * channels * ells,
        traffic=4 * own.size + 2 * wide * channels * ells,
        vmem=16,
    )(*operands)


def finish_body(columns, pairs, maps, tile, order_ref, *refs):
    ins, (harm_ref, power_ref) = refs[:-2], refs[-2:]
    channels = 2 * maps
    start = pl.program_id(0) * tile
    total = [None] * maps
    part = ins[0].shape[0]
    ell = start + lax.broadcasted_iota(jnp.int32, (part, tile), 1)
    for c in range(pairs):
        mine = ins[c * columns : (c + 1) * columns]
        value = mine[0][...]
        for other in mine[1:]:
            value = value + other[...].astype(jnp.float32)
        order = order_ref[c * part : (c + 1) * part, 0:1]
        value = jnp.where(ell >= order, value, 0.0)
        harm_ref[c * part : (c + 1) * part, :] = value
        weighted = jnp.where(order == 0, value, 2.0 * value)
        for s in range(part // channels):
            mode = value[s * channels : (s + 1) * channels]
            heavy = weighted[s * channels : (s + 1) * channels]
            for k in range(maps // 2 + 1):
                turned = mode if k == 0 else jnp.concatenate([mode[2 * k :], mode[: 2 * k]], axis=0)
                term = heavy * turned
                total[k] = term if total[k] is None else total[k] + term
    pair = 0
    for i in range(maps):
        for j in range(i, maps):
            k, a = (j - i, i) if j - i <= maps // 2 else (maps - (j - i), j)
            power_ref[pair : pair + 1, :] = total[k][2 * a : 2 * a + 1] + total[k][2 * a + 1 : 2 * a + 2]
            pair += 1


def finish(columns, pairs_in, maps, orders, parts):
    ells = parts[0].shape[1]
    part = parts[0].shape[0]
    tile = ells // 4
    pairs = maps * (maps + 1) // 2
    rows = part * pairs_in
    return kernel_call(
        functools.partial(finish_body, columns, pairs_in, maps, tile),
        [jax.ShapeDtypeStruct((rows, ells), jnp.float32), jax.ShapeDtypeStruct((pairs, ells), jnp.float32)],
        grid=(ells // tile,),
        in_specs=[pl.BlockSpec((rows, 128), lambda t: (0, 0))]
        + [pl.BlockSpec((part, tile), lambda t: (0, t))] * len(parts),
        out_specs=[pl.BlockSpec((rows, tile), lambda t: (0, t)), pl.BlockSpec((pairs, tile), lambda t: (0, t))],
        flops=20 * rows * ells,
        traffic=4 * rows * ells * 4,
        vmem=10,
    )(orders, *parts)


def per_device(sky_maps, legendre, owner_table):
    maps = sky_maps.shape[0]
    cycles, order_count, ells = legendre.shape
    devices = lax.axis_size(AXES)
    columns = devices // PLANE
    own_count = order_count // devices
    chunks = min(CHUNKS, own_count)
    share = own_count // chunks
    pairs = chunks // 2
    size = columns * share
    wide = 2 * size
    channels = 2 * maps
    me = lax.axis_index(AXES)

    core, chunk, one, two, step, item = np.indices((2, chunks, 2, 2, columns, share)).reshape(6, -1)
    swap = chunk % 2 == 1
    low = core + 2 * np.where(swap, two, one) + 4 * np.where(swap, one, two)
    member = (me % PLANE) ^ jnp.asarray(low, jnp.int32)
    column = (me // PLANE + jnp.asarray(step, jnp.int32)) % columns
    slot = (column * PLANE + member) * own_count + jnp.asarray(chunk * share + item, jnp.int32)
    index = lax.iota(jnp.int32, order_count)
    order = jnp.sum(jnp.where(slot[:, None] == index[None, :], owner_table[None, :], 0), axis=1)
    one_hot = (order[:, None] == index[None, :]).astype(jnp.bfloat16)

    def swap_with(value, bit):
        return lax.ppermute(value, AXES, [(d, d ^ bit) for d in range(devices)])

    def send_all(values, send):
        done = []
        for i, value in enumerate(values):
            done.append(send(i, value))
        return done

    per_pair = 8 * size
    early = pairs // 2
    out_early = permute_rows(one_hot, 2, early, per_pair, legendre)
    got = [swap_with(value, 1) for value in out_early]
    four = owned_fourier(sky_maps, one_hot)
    half = order_count // 2
    own = permute_rows(one_hot, 0, early, per_pair, legendre)
    coef = jnp.stack([four[:, :, :half], swap_with(four[:, :, half:], 1)])
    coef = coef.reshape(2, 2, maps, cycles, half // wide, wide)
    coef = jnp.transpose(coef, (4, 2, 1, 0, 3, 5)).reshape(half // wide, channels, 2 * cycles * wide)

    wire = jnp.bfloat16
    rows = size * channels
    part = share * channels

    firsts, seconds, parts, last = {}, {}, [], [None]

    def stage(body, p, adds, outs):
        made = pair_stage(body, wide, p, coef, own[p], got[p], adds, outs, last[0])
        last[0] = made[0]
        return made

    def first_stage(p):
        sends = stage(first_body, p, [], [(2 * rows, wire)] * 2)
        firsts[p] = send_all(sends, lambda i, send: swap_with(send, (2, 4)[i]))

    def second_stage(p):
        adds = [(value, 1, rows) for value in firsts[p]]
        sends = stage(second_body, p, adds, [(rows, wire)] * 2)
        seconds[p] = send_all(sends, lambda i, send: swap_with(send, (4, 2)[i]))

    def last_stage(p):
        adds = [(value, 0, rows) for value in firsts[p] + seconds[p]]
        outs = [(2 * part, jnp.float32)] + [(2 * part, wire)] * (columns - 1)
        keep, *sends = stage(last_body, p, adds, outs)
        rings = [[(d, (d + k * PLANE) % devices) for d in range(devices)] for k in range(1, columns)]
        parts.append([keep] + send_all(sends, lambda i, send: lax.ppermute(send, AXES, rings[i])))

    for p in range(early):
        first_stage(p)
    out_late = permute_rows(one_hot, 3, pairs - early, per_pair, legendre, last[0])
    got += send_all(out_late, lambda i, value: swap_with(value, 1))
    own = list(own) + list(permute_rows(one_hot, 1, pairs - early, per_pair, legendre, out_late[0]))
    last[0] = own[-1]
    ahead = 2
    for p in range(early, min(ahead, pairs)):
        first_stage(p)
    for p in range(pairs + 1):
        if p < pairs:
            second_stage(p)
        if max(early, ahead) <= p + ahead < pairs:
            first_stage(p + ahead)
        if p > 0:
            last_stage(p - 1)
    parts = [piece for group in parts for piece in group]

    owned = lax.dynamic_slice_in_dim(owner_table, me * own_count, own_count)
    orders = jnp.broadcast_to(owned[:, None, None], (own_count, channels, 128)).reshape(-1, 128)
    harmonics, power = finish(columns, pairs, maps, orders, parts)
    harmonics = harmonics.reshape(own_count, maps, 2, ells)
    ell_share = ells // devices
    spread = power.reshape(power.shape[0], devices, ell_share).transpose(1, 0, 2)
    shares = lax.all_to_all(spread, AXES, split_axis=0, concat_axis=0, tiled=True)
    owned_ells = me * ell_share + lax.iota(jnp.int32, ell_share)
    spectra = jnp.sum(shares, axis=0) / (2 * owned_ells + 1).astype(jnp.float32)[None, :]
    return (harmonics, spectra)


def solution(mesh):
    return jax.shard_map(
        per_device,
        mesh=mesh,
        in_specs=(P(None, AXES, None), P(AXES, None, None), P()),
        out_specs=(P(AXES, None, None, None), P(None, AXES)),
        check_vma=False,
    )
```
